32 devices in a mesh: slab: 8 (over y, x, core), det: 4 (over z).
Axes of the slice: x: 2, y: 2, z: 4, core: 2. Of those that a mesh axis runs over, the one named last changes fastest.
Arguments:
- traces: float32 [32, 128, 4096], P(('slab', 'det')), may hold values from -6 to 6
- tables: bfloat16 [32, 256, 2048], P('slab', None, 'det'), may hold values from -0.0625 to 0.0625
- slab_range: int32 [32, 2], P(('slab', 'det')), may hold values from 0 to 7, as said below
- table_slot: int32 [32, 7], P(('slab', 'det')), may hold values from 0 to 3
- sample_start: int32 [32, 7], P(('slab', 'det')), may hold values from 0 to 3840
Outputs:
- image: float32 [128, 16384], P(None, ('slab', 'det'))
The draws below stay inside these ranges and needn't reach their ends.
Inputs may be any that keep to these rules, and one draw needn't show every extreme that they name: For detector d with home slab g = d // 4: max(0, g - 3) <= slab_range[d, 0] <= g <= slab_range[d, 1] <= min(7, g + 3); some detectors reach the full 3 on both sides where the grid allows.
All inputs are finite; a program needn't handle non-finite values.
Results may differ from the reference program's by a relative error of at most 0.007.
Values may be sent and summed in bfloat16 or wider, within the bound.
A program may use at most 64 MiB of HBM per device.

```python
import jax
import jax.numpy as jnp
from jax import lax

SAMP = 4096
KWIN = 256
NTAB = 4
RANGE = 3
VOX = 2048
FRAMES = 128
DET_DEV = 1
DETS = 32
N_SLAB = 8
N_DET = 4


def draw_slab_range(key, part):
    lower_key, upper_key = jax.random.split(jax.random.fold_in(key, 11))
    detector_index = jnp.arange(DETS, dtype=jnp.int32)
    home = detector_index // (N_DET * DET_DEV)
    lower_reach = jax.random.randint(lower_key, (DETS,), 0, RANGE + 1)
    upper_reach = jax.random.randint(upper_key, (DETS,), 0, RANGE + 1)
    widest = detector_index % 7 == 0
    lower_reach = jnp.where(widest, RANGE, lower_reach)
    upper_reach = jnp.where(widest, RANGE, upper_reach)
    first_slab = jnp.maximum(home - lower_reach, 0)
    last_slab = jnp.minimum(home + upper_reach, N_SLAB - 1)
    return jnp.stack([first_slab, last_slab], axis=1).astype(jnp.int32)


def plant(entries, rng, smallest, largest):
    longest = entries.shape.index(max(entries.shape))
    spots = []
    for shift in (0, 1):
        where = [jax.random.randint(jax.random.fold_in(rng, axis), (), 0, length) for axis, length in enumerate(entries.shape)]
        where[longest] = (where[longest] + shift) % entries.shape[longest]
        spots.append(tuple(where))
    return entries.at[spots[0]].set(smallest).at[spots[1]].set(largest)


def block_levels(key, shape, cuts, smallest, top_value):
    def one(dim, parts):
        steps = jax.random.uniform(jax.random.fold_in(jax.random.fold_in(key, 6), dim), (parts,), jnp.float32, smallest / len(cuts), top_value / len(cuts))
        return jnp.repeat(jnp.exp(steps), shape[dim] // parts).reshape((-1,) + (1,) * (len(shape) - dim - 1))

    loudness = one(*cuts[0])
    for cut in cuts[1:]:
        loudness = loudness * one(*cut)
    return loudness


def normal_values(key, shape, deviation, bound, cuts=(), kind=jnp.bfloat16):
    array = jax.random.normal(key, shape, jnp.float32) * deviation
    if len(cuts) > 0:
        array = block_levels(key, shape, cuts, -0.22, 0.18) * array
    return jnp.clip(array, min=-bound, max=bound).astype(kind)


def setup_inputs(seed: int = 0) -> dict:
    splits = jax.random.split(jax.random.key(seed), 6)
    traces = normal_values(splits[0], (DETS, FRAMES, SAMP), 1.0, 6.0, ((0, 32),), jnp.float32)
    tables = normal_values(splits[1], (N_SLAB * NTAB, KWIN, N_SLAB * 0 + VOX), (4 * (2 * RANGE + 1) * DET_DEV * KWIN) ** -0.5, 0.0625, ((0, 8), (2, 4)))
    slab_range = draw_slab_range(jax.random.fold_in(splits[5], 71), 0)
    table_slot = plant(jax.random.randint(splits[3], (DETS, 2 * RANGE + 1), 0, NTAB), jax.random.fold_in(splits[3], 1), 0, NTAB - 1).astype(jnp.int32)
    sample_start = plant(jax.random.randint(splits[4], (DETS, 2 * RANGE + 1), 0, SAMP - KWIN + 1), jax.random.fold_in(splits[4], 1), 0, SAMP - KWIN).astype(jnp.int32)
    return {"traces": traces, "tables": tables, "slab_range": slab_range, "table_slot": table_slot, "sample_start": sample_start}


def windows_for(trace_rows, starts):
    def single(trace_row, first_index):
        return lax.dynamic_slice_in_dim(trace_row, first_index, KWIN, 1)
    return jax.vmap(single)(trace_rows, starts)


def reference(traces, tables, slab_range, table_slot, sample_start):
    group = N_DET * DET_DEV
    table_blocks = tables.reshape(N_SLAB, NTAB, KWIN, VOX)
    slot_values = jnp.arange(NTAB, dtype=jnp.int32)

    def one_slab(slab):
        stacked = jnp.zeros((N_DET, NTAB, FRAMES, KWIN), jnp.float32)
        for offset in range(-RANGE, RANGE + 1):
            home = slab - offset
            valid = (home >= 0) & (home < N_SLAB)
            clipped = jnp.clip(home, 0, N_SLAB - 1)
            first_row = (clipped * group).astype(jnp.int32)
            trace_rows = lax.dynamic_slice_in_dim(traces, first_row, group, 0).astype(jnp.bfloat16)
            ranges = lax.dynamic_slice_in_dim(slab_range, first_row, group, 0)
            slot_ids = lax.dynamic_slice_in_dim(table_slot, first_row, group, 0)[:, offset + RANGE]
            starts = lax.dynamic_slice_in_dim(sample_start, first_row, group, 0)[:, offset + RANGE]
            active = valid & (ranges[:, 0] <= slab) & (slab <= ranges[:, 1])
            windows = windows_for(trace_rows, starts).astype(jnp.float32)
            windows = windows.reshape(N_DET, DET_DEV, FRAMES, KWIN)
            onehot = ((slot_ids[:, None] == slot_values[None, :]) & active[:, None]).astype(jnp.float32)
            onehot = onehot.reshape(N_DET, DET_DEV, NTAB)
            stacked = stacked + jnp.einsum("kit,kifw->ktfw", onehot, windows)
        rounded = stacked.astype(jnp.bfloat16).astype(jnp.float32)
        weights = table_blocks[slab].astype(jnp.float32)
        return jnp.einsum("ktfw,twv->fv", rounded, weights)

    slabs = lax.map(one_slab, jnp.arange(N_SLAB, dtype=jnp.int32))
    return jnp.transpose(slabs, (1, 0, 2)).reshape(FRAMES, N_SLAB * VOX)
```

```python
import functools

import jax
import jax.numpy as jnp
from jax import lax
from jax.experimental import pallas as pl
from jax.experimental.pallas import tpu as pltpu
from jax.sharding import PartitionSpec as P

MESH = pl.DeviceIdType.MESH
KWIN = 256
NTAB = 4
RANGE = 3
LANES = 128
OFFSETS = 2 * RANGE + 1


def cut_kernel(n_slab, traces, slab_range, table_slot, sample_start, wins, masks, spans, sems):
    slab = lax.axis_index("slab")
    samp, span = traces.shape[2], spans.shape[2]
    n_quarter, _, rows, _ = wins.shape
    loads, inner = [], []
    for o in range(OFFSETS):
        start = sample_start[0, o]
        tile = jnp.minimum(lax.div(start, LANES), (samp - span) // LANES)
        inner.append(start - tile * LANES)
        first = pl.multiple_of(tile * LANES, LANES)
        loads.append(
            pltpu.make_async_copy(traces.at[0, :, pl.ds(first, span)], spans.at[o], sems.at[o])
        )
        loads[-1].start()
    mask_rows = lax.broadcasted_iota(jnp.int32, masks.shape[1:], 0)
    for o in range(OFFSETS):
        target = slab + (o - RANGE)
        active = (slab_range[0, 0] <= target) & (target <= slab_range[0, 1])
        slot = jnp.where(active, table_slot[0, o], -1)
        masks[o] = (mask_rows == slot).astype(jnp.float32)
    far = lax.broadcasted_iota(jnp.int32, (span, KWIN), 0)
    far = far - lax.broadcasted_iota(jnp.int32, (span, KWIN), 1)
    for o in range(OFFSETS):
        pick = (far == inner[o]).astype(jnp.bfloat16)
        loads[o].wait()
        moved = jnp.dot(spans[o].astype(jnp.bfloat16), pick, preferred_element_type=jnp.float32)
        for q in range(n_quarter):
            wins[q, o] = moved[q * rows : (q + 1) * rows].astype(jnp.bfloat16)


def kernel(
    n_slab, n_det,
    send_win, send_mask, tables, out,
    table_buf, got_win, got_mask,
    part, got_part, total, got_total,
    table_sem, win_send, win_recv, mask_send, mask_recv,
    part_send, part_recv, total_send, total_recv,
):
    slab, det = lax.axis_index("slab"), lax.axis_index("det")
    rows = send_win.shape[2]
    order = sorted(range(1, n_det), key=lambda d: -min(d, n_det - d)) + [0]
    away = [o for o in range(OFFSETS) if o != RANGE]
    away.sort(key=lambda o: -abs(o - RANGE))

    def valid(to):
        return (to >= 0) & (to < n_slab)

    def part_of(d):
        return lax.rem(det + d, n_det)

    table_load = pltpu.make_async_copy(tables, table_buf, table_sem)
    table_load.start()

    barrier = pltpu.get_barrier_semaphore()
    peers = jnp.int32(n_det - 1)
    for o in away:
        peer = slab + (o - RANGE)
        peers = peers + valid(peer).astype(jnp.int32)

        @pl.when(valid(peer))
        def _():
            pl.semaphore_signal(barrier, 1, device_id=(peer, det), device_id_type=MESH)

    for d in order[:-1]:
        pl.semaphore_signal(
            barrier, 1, device_id=(slab, part_of(d)), device_id_type=MESH
        )

    def mask_copy(o):
        return pltpu.make_async_remote_copy(
            src_ref=send_mask.at[o], dst_ref=got_mask.at[o],
            send_sem=mask_send.at[o], recv_sem=mask_recv.at[o],
            device_id=(slab + (o - RANGE), det), device_id_type=MESH,
        )

    def win_copy(c, o):
        return pltpu.make_async_remote_copy(
            src_ref=send_win.at[part_of(order[c]), o], dst_ref=got_win.at[c, o],
            send_sem=win_send.at[c, o], recv_sem=win_recv.at[c, o],
            device_id=(slab + (o - RANGE), det), device_id_type=MESH,
        )

    def part_copy(c):
        d = order[c]
        return pltpu.make_async_remote_copy(
            src_ref=part.at[c], dst_ref=got_part.at[c],
            send_sem=part_send.at[c], recv_sem=part_recv.at[c],
            device_id=(slab, part_of(d)), device_id_type=MESH,
        )

    def total_copy(c):
        d = order[c]
        return pltpu.make_async_remote_copy(
            src_ref=total, dst_ref=got_total.at[c],
            send_sem=total_send.at[c], recv_sem=total_recv.at[c],
            device_id=(slab, part_of(d)), device_id_type=MESH,
        )

    pl.semaphore_wait(barrier, peers)
    for c in range(n_det):
        for o in away:

            @pl.when(valid(slab + (o - RANGE)))
            def _():
                if c == 0:
                    mask_copy(o).start()
                win_copy(c, o).start()

    for o in away:

        @pl.when(jnp.logical_not(valid(slab - (o - RANGE))))
        def _():
            got_mask[o] = jnp.zeros(got_mask.shape[1:], got_mask.dtype)
            for c in range(n_det):
                got_win[c, o] = jnp.zeros(got_win.shape[2:], got_win.dtype)

    for c in range(n_det):
        for o in away:

            @pl.when(valid(slab - (o - RANGE)))
            def _():
                if c == 0:
                    mask_copy(o).wait_recv()
                win_copy(c, o).wait_recv()

        bins = [jnp.zeros((rows, KWIN), jnp.float32) for _ in range(NTAB)]
        for o in range(OFFSETS):
            if o == RANGE:
                win, mask = send_win[part_of(order[c]), o], send_mask
            else:
                win, mask = got_win[c, o], got_mask
            win = win.astype(jnp.float32)
            for t in range(NTAB):
                bins[t] = bins[t] + mask[o, t : t + 1] * win
        for t in range(NTAB):
            part[c, :, t * KWIN : (t + 1) * KWIN] = bins[t].astype(jnp.bfloat16)
        if order[c] != 0:
            part_copy(c).start()

    summed = part[n_det - 1].astype(jnp.float32)
    for c in range(n_det - 1):
        part_copy(c).wait_recv()
        summed = summed + got_part[c].astype(jnp.float32)
    total[...] = summed.astype(jnp.bfloat16)
    for c in range(n_det - 1):
        total_copy(c).start()

    table_load.wait()
    weights = table_buf[...].reshape(NTAB * KWIN, table_buf.shape[2])

    def finish(quarter_sum, d):
        out[pl.ds(pl.multiple_of(part_of(d) * rows, rows), rows), :] = jnp.dot(
            quarter_sum, weights, preferred_element_type=jnp.float32
        )

    finish(total[...], 0)
    nearest = sorted(range(n_det - 1), key=lambda c: min(order[c], n_det - order[c]))
    for c in nearest:
        total_copy(c).wait_recv()
        finish(got_total[c], n_det - order[c])

    for o in away:

        @pl.when(valid(slab + (o - RANGE)))
        def _():
            mask_copy(o).wait_send()
            for c in range(n_det):
                win_copy(c, o).wait_send()

    for c in range(n_det - 1):
        part_copy(c).wait_send()
        total_copy(c).wait_send()


def body(n_slab, n_det, traces, tables, slab_range, table_slot, sample_start):
    _, frames, samp = traces.shape
    voxels = tables.shape[2]
    rows = frames // n_det
    wide = NTAB * KWIN
    mask_rows = -(-NTAB // 8) * 8
    anywhere = pl.BlockSpec(memory_space=pl.ANY)
    scalars = pl.BlockSpec(memory_space=pltpu.SMEM)
    vmem = pl.BlockSpec(memory_space=pltpu.VMEM)
    dma = pltpu.SemaphoreType.DMA
    wins, masks = pl.pallas_call(
        functools.partial(cut_kernel, n_slab),
        out_shape=[
            jax.ShapeDtypeStruct((n_det, OFFSETS, rows, KWIN), jnp.bfloat16),
            jax.ShapeDtypeStruct((OFFSETS, mask_rows, KWIN), jnp.float32),
        ],
        in_specs=[pl.BlockSpec(memory_space=pltpu.HBM), scalars, scalars, scalars],
        out_specs=[vmem, vmem],
        scratch_shapes=[
            pltpu.VMEM((OFFSETS, frames, KWIN + LANES), jnp.float32),
            dma((OFFSETS,)),
        ],
        compiler_params=pltpu.CompilerParams(vmem_limit_bytes=16 * 1024 * 1024),
    )(traces, slab_range, table_slot, sample_start)
    return pl.pallas_call(
        functools.partial(kernel, n_slab, n_det),
        out_shape=jax.ShapeDtypeStruct((frames, voxels), jnp.float32),
        in_specs=[vmem, vmem, anywhere],
        out_specs=vmem,
        scratch_shapes=[
            pltpu.VMEM(tables.shape, jnp.bfloat16),
            pltpu.VMEM((n_det, OFFSETS, rows, KWIN), jnp.bfloat16),
            pltpu.VMEM((OFFSETS, mask_rows, KWIN), jnp.float32),
            pltpu.VMEM((n_det, rows, wide), jnp.bfloat16),
            pltpu.VMEM((n_det, rows, wide), jnp.bfloat16),
            pltpu.VMEM((rows, wide), jnp.bfloat16),
            pltpu.VMEM((n_det, rows, wide), jnp.bfloat16),
            dma,
            dma((n_det, OFFSETS)),
            dma((n_det, OFFSETS)),
            dma((OFFSETS,)),
            dma((OFFSETS,)),
            dma((n_det,)),
            dma((n_det,)),
            dma((n_det,)),
            dma((n_det,)),
        ],
        compiler_params=pltpu.CompilerParams(
            collective_id=0, has_side_effects=True, vmem_limit_bytes=16 * 1024 * 1024
        ),
    )(wins, masks, tables)


def solution(mesh):
    placed = (
        P(("slab", "det"), None, None),
        P("slab", None, "det"),
        P(("slab", "det"), None),
        P(("slab", "det"), None),
        P(("slab", "det"), None),
    )
    return jax.shard_map(
        functools.partial(body, mesh.shape["slab"], mesh.shape["det"]),
        mesh=mesh, in_specs=placed, out_specs=P(None, ("slab", "det")), check_vma=False,
    )
```

```python
import functools

import jax
import jax.numpy as jnp
from jax import lax
from jax.experimental import pallas as pl
from jax.experimental.pallas import tpu as pltpu
from jax.sharding import PartitionSpec as P

MESH = pl.DeviceIdType.MESH
KWIN = 256
NTAB = 4
RANGE = 3
LANES = 128
OFFSETS = 2 * RANGE + 1


def cut_kernel(n_slab, traces, slab_range, table_slot, sample_start, wins, masks, spans, cuts, mask_buf, sems, out_sems):
    slab = lax.axis_index("slab")
    samp, span = traces.shape[2], spans.shape[2]
    _, n_quarter, rows, _ = wins.shape
    loads, inner = [], []
    for o in range(OFFSETS):
        start = sample_start[0, o]
        tile = jnp.minimum(lax.div(start, LANES), (samp - span) // LANES)
        inner.append(start - tile * LANES)
        first = pl.multiple_of(tile * LANES, LANES)
        loads.append(
            pltpu.make_async_copy(traces.at[0, :, pl.ds(first, span)], spans.at[o], sems.at[o])
        )
        loads[-1].start()
    mask_rows = lax.broadcasted_iota(jnp.int32, mask_buf.shape[1:], 0)
    for o in range(OFFSETS):
        target = slab + (o - RANGE)
        active = (slab_range[0, 0] <= target) & (target <= slab_range[0, 1])
        slot = jnp.where(active, table_slot[0, o], -1)
        mask_buf[o] = (mask_rows == slot).astype(jnp.float32)
    stores = [pltpu.make_async_copy(mask_buf, masks, out_sems.at[OFFSETS])]
    stores[0].start()
    far = lax.broadcasted_iota(jnp.int32, (span, KWIN), 0)
    far = far - lax.broadcasted_iota(jnp.int32, (span, KWIN), 1)
    for o in range(OFFSETS):
        pick = (far == inner[o]).astype(jnp.bfloat16)
        loads[o].wait()
        moved = jnp.dot(spans[o].astype(jnp.bfloat16), pick, preferred_element_type=jnp.float32)
        for q in range(n_quarter):
            cuts[o, q] = moved[q * rows : (q + 1) * rows].astype(jnp.bfloat16)
        stores.append(pltpu.make_async_copy(cuts.at[o], wins.at[o], out_sems.at[o]))
        stores[-1].start()
    for store in stores:
        store.wait()


def kernel(
    n_slab, n_det,
    wins, masks, tables, out,
    send_win, send_mask, table_buf, got_win, got_mask,
    part, got_part, total, got_total,
    win_load, mask_load, table_sem, win_send, win_recv, mask_send, mask_recv,
    part_send, part_recv, total_send, total_recv,
):
    slab, det = lax.axis_index("slab"), lax.axis_index("det")
    rows = send_win.shape[2]
    order = sorted(range(1, n_det), key=lambda d: -min(d, n_det - d)) + [0]
    away = [o for o in range(OFFSETS) if o != RANGE]
    away.sort(key=lambda o: -abs(o - RANGE))

    def valid(to):
        return (to >= 0) & (to < n_slab)

    def part_of(d):
        return lax.rem(det + d, n_det)

    loads = [
        pltpu.make_async_copy(masks, send_mask, mask_load),
        pltpu.make_async_copy(wins, send_win, win_load),
    ]
    for load in loads:
        load.start()
    table_load = pltpu.make_async_copy(tables, table_buf, table_sem)
    table_load.start()

    barrier = pltpu.get_barrier_semaphore()
    peers = jnp.int32(n_det - 1)
    for o in away:
        peer = slab + (o - RANGE)
        peers = peers + valid(peer).astype(jnp.int32)

        @pl.when(valid(peer))
        def _():
            pl.semaphore_signal(barrier, 1, device_id=(peer, det), device_id_type=MESH)

    for d in order[:-1]:
        pl.semaphore_signal(
            barrier, 1, device_id=(slab, part_of(d)), device_id_type=MESH
        )

    def mask_copy(o):
        return pltpu.make_async_remote_copy(
            src_ref=send_mask.at[o], dst_ref=got_mask.at[o],
            send_sem=mask_send.at[o], recv_sem=mask_recv.at[o],
            device_id=(slab + (o - RANGE), det), device_id_type=MESH,
        )

    def win_copy(c, o):
        return pltpu.make_async_remote_copy(
            src_ref=send_win.at[o, part_of(order[c])], dst_ref=got_win.at[c, o],
            send_sem=win_send.at[c, o], recv_sem=win_recv.at[c, o],
            device_id=(slab + (o - RANGE), det), device_id_type=MESH,
        )

    def part_copy(c):
        d = order[c]
        return pltpu.make_async_remote_copy(
            src_ref=part.at[c], dst_ref=got_part.at[c],
            send_sem=part_send.at[c], recv_sem=part_recv.at[c],
            device_id=(slab, part_of(d)), device_id_type=MESH,
        )

    def total_copy(c):
        d = order[c]
        return pltpu.make_async_remote_copy(
            src_ref=total, dst_ref=got_total.at[c],
            send_sem=total_send.at[c], recv_sem=total_recv.at[c],
            device_id=(slab, part_of(d)), device_id_type=MESH,
        )

    for load in loads:
        load.wait()
    pl.semaphore_wait(barrier, peers)
    for c in range(n_det):
        for o in away:

            @pl.when(valid(slab + (o - RANGE)))
            def _():
                if c == 0:
                    mask_copy(o).start()
                win_copy(c, o).start()

    for o in away:

        @pl.when(jnp.logical_not(valid(slab - (o - RANGE))))
        def _():
            got_mask[o] = jnp.zeros(got_mask.shape[1:], got_mask.dtype)
            for c in range(n_det):
                got_win[c, o] = jnp.zeros(got_win.shape[2:], got_win.dtype)

    for c in range(n_det):
        for o in away:

            @pl.when(valid(slab - (o - RANGE)))
            def _():
                if c == 0:
                    mask_copy(o).wait_recv()
                win_copy(c, o).wait_recv()

        bins = [jnp.zeros((rows, KWIN), jnp.float32) for _ in range(NTAB)]
        for o in range(OFFSETS):
            if o == RANGE:
                win, mask = send_win[o, part_of(order[c])], send_mask
            else:
                win, mask = got_win[c, o], got_mask
            win = win.astype(jnp.float32)
            for t in range(NTAB):
                bins[t] = bins[t] + mask[o, t : t + 1] * win
        for t in range(NTAB):
            part[c, :, t * KWIN : (t + 1) * KWIN] = bins[t].astype(jnp.bfloat16)
        if order[c] != 0:
            part_copy(c).start()

    summed = part[n_det - 1].astype(jnp.float32)
    for c in range(n_det - 1):
        part_copy(c).wait_recv()
        summed = summed + got_part[c].astype(jnp.float32)
    total[...] = summed.astype(jnp.bfloat16)
    for c in range(n_det - 1):
        total_copy(c).start()

    table_load.wait()
    weights = table_buf[...].reshape(NTAB * KWIN, table_buf.shape[2])

    def finish(quarter_sum, d):
        out[pl.ds(pl.multiple_of(part_of(d) * rows, rows), rows), :] = jnp.dot(
            quarter_sum, weights, preferred_element_type=jnp.float32
        )

    finish(total[...], 0)
    nearest = sorted(range(n_det - 1), key=lambda c: min(order[c], n_det - order[c]))
    for c in nearest:
        total_copy(c).wait_recv()
        finish(got_total[c], n_det - order[c])

    for o in away:

        @pl.when(valid(slab + (o - RANGE)))
        def _():
            mask_copy(o).wait_send()
            for c in range(n_det):
                win_copy(c, o).wait_send()

    for c in range(n_det - 1):
        part_copy(c).wait_send()
        total_copy(c).wait_send()


def body(n_slab, n_det, traces, tables, slab_range, table_slot, sample_start):
    _, frames, samp = traces.shape
    voxels = tables.shape[2]
    rows = frames // n_det
    wide = NTAB * KWIN
    mask_rows = -(-NTAB // 8) * 8
    anywhere = pl.BlockSpec(memory_space=pl.ANY)
    scalars = pl.BlockSpec(memory_space=pltpu.SMEM)
    vmem = pl.BlockSpec(memory_space=pltpu.VMEM)
    dma = pltpu.SemaphoreType.DMA
    wins, masks = pl.pallas_call(
        functools.partial(cut_kernel, n_slab),
        out_shape=[
            jax.ShapeDtypeStruct((OFFSETS, n_det, rows, KWIN), jnp.bfloat16),
            jax.ShapeDtypeStruct((OFFSETS, mask_rows, KWIN), jnp.float32),
        ],
        in_specs=[anywhere, scalars, scalars, scalars],
        out_specs=[anywhere, anywhere],
        scratch_shapes=[
            pltpu.VMEM((OFFSETS, frames, KWIN + LANES), jnp.float32),
            pltpu.VMEM((OFFSETS, n_det, rows, KWIN), jnp.bfloat16),
            pltpu.VMEM((OFFSETS, mask_rows, KWIN), jnp.float32),
            dma((OFFSETS,)),
            dma((OFFSETS + 1,)),
        ],
    )(traces, slab_range, table_slot, sample_start)
    return pl.pallas_call(
        functools.partial(kernel, n_slab, n_det),
        out_shape=jax.ShapeDtypeStruct((frames, voxels), jnp.float32),
        in_specs=[anywhere, anywhere, anywhere],
        out_specs=vmem,
        scratch_shapes=[
            pltpu.VMEM((OFFSETS, n_det, rows, KWIN), jnp.bfloat16),
            pltpu.VMEM((OFFSETS, mask_rows, KWIN), jnp.float32),
            pltpu.VMEM(tables.shape, jnp.bfloat16),
            pltpu.VMEM((n_det, OFFSETS, rows, KWIN), jnp.bfloat16),
            pltpu.VMEM((OFFSETS, mask_rows, KWIN), jnp.float32),
            pltpu.VMEM((n_det, rows, wide), jnp.bfloat16),
            pltpu.VMEM((n_det, rows, wide), jnp.bfloat16),
            pltpu.VMEM((rows, wide), jnp.bfloat16),
            pltpu.VMEM((n_det, rows, wide), jnp.bfloat16),
            dma,
            dma,
            dma,
            dma((n_det, OFFSETS)),
            dma((n_det, OFFSETS)),
            dma((OFFSETS,)),
            dma((OFFSETS,)),
            dma((n_det,)),
            dma((n_det,)),
            dma((n_det,)),
            dma((n_det,)),
        ],
        compiler_params=pltpu.CompilerParams(
            collective_id=0, has_side_effects=True
        ),
    )(wins, masks, tables)


def solution(mesh):
    placed = (
        P(("slab", "det"), None, None),
        P("slab", None, "det"),
        P(("slab", "det"), None),
        P(("slab", "det"), None),
        P(("slab", "det"), None),
    )
    return jax.shard_map(
        functools.partial(body, mesh.shape["slab"], mesh.shape["det"]),
        mesh=mesh, in_specs=placed, out_specs=P(None, ("slab", "det")), check_vma=False,
    )
```

```python
import functools

import jax
import jax.numpy as jnp
from jax import lax
from jax.experimental import pallas as pl
from jax.experimental.pallas import tpu as pltpu
from jax.sharding import PartitionSpec as P

MESH = pl.DeviceIdType.MESH
KWIN = 256
NTAB = 4
RANGE = 3
LANES = 128
OFFSETS = 2 * RANGE + 1
CUT_LIMIT = 16 * 1024 * 1024


def cut_kernel(n_slab, traces, whole, wins, masks, spans, sems):
    slab = lax.axis_index("slab")
    samp, span = traces.shape[2], spans.shape[2]
    n_quarter, _, rows, _ = wins.shape
    loads, inner = [], []
    for o in range(OFFSETS):
        start = whole[0, 2 + OFFSETS + o]
        tile = jnp.minimum(lax.div(start, LANES), (samp - span) // LANES)
        inner.append(start - tile * LANES)
        first = pl.multiple_of(tile * LANES, LANES)
        loads.append(
            pltpu.make_async_copy(traces.at[0, :, pl.ds(first, span)], spans.at[o], sems.at[o])
        )
        loads[-1].start()
    mask_rows = lax.broadcasted_iota(jnp.int32, masks.shape[1:], 0)
    for o in range(OFFSETS):
        target = slab + (o - RANGE)
        active = (whole[0, 0] <= target) & (target <= whole[0, 1])
        slot = jnp.where(active, whole[0, 2 + o], -1)
        masks[o] = (mask_rows == slot).astype(jnp.float32)
    far = lax.broadcasted_iota(jnp.int32, (span, KWIN), 0)
    far = far - lax.broadcasted_iota(jnp.int32, (span, KWIN), 1)
    for o in range(OFFSETS):
        pick = (far == inner[o]).astype(jnp.bfloat16)
        loads[o].wait()
        moved = jnp.dot(spans[o].astype(jnp.bfloat16), pick, preferred_element_type=jnp.float32)
        for q in range(n_quarter):
            wins[q, o] = moved[q * rows : (q + 1) * rows].astype(jnp.bfloat16)


def kernel(
    n_slab, n_det,
    send_win, send_mask, tables, out,
    table_buf, got_win, got_mask,
    part, got_part, total, got_total,
    table_sem, win_send, win_recv, mask_send, mask_recv,
    part_send, part_recv, total_send, total_recv,
):
    slab, det = lax.axis_index("slab"), lax.axis_index("det")
    rows = send_win.shape[2]
    order = sorted(range(1, n_det), key=lambda d: -min(d, n_det - d)) + [0]
    away = [o for o in range(OFFSETS) if o != RANGE]
    away.sort(key=lambda o: -abs(o - RANGE))

    def valid(to):
        return (to >= 0) & (to < n_slab)

    def part_of(d):
        return lax.rem(det + d, n_det)

    table_load = pltpu.make_async_copy(tables, table_buf, table_sem)
    table_load.start()

    barrier = pltpu.get_barrier_semaphore()
    peers = jnp.int32(n_det - 1)
    for o in away:
        peer = slab + (o - RANGE)
        peers = peers + valid(peer).astype(jnp.int32)

        @pl.when(valid(peer))
        def _():
            pl.semaphore_signal(barrier, 1, device_id=(peer, det), device_id_type=MESH)

    for d in order[:-1]:
        pl.semaphore_signal(
            barrier, 1, device_id=(slab, part_of(d)), device_id_type=MESH
        )

    def mask_copy(o):
        return pltpu.make_async_remote_copy(
            src_ref=send_mask.at[o], dst_ref=got_mask.at[o],
            send_sem=mask_send.at[o], recv_sem=mask_recv.at[o],
            device_id=(slab + (o - RANGE), det), device_id_type=MESH,
        )

    def win_copy(c, o):
        return pltpu.make_async_remote_copy(
            src_ref=send_win.at[part_of(order[c]), o], dst_ref=got_win.at[c, o],
            send_sem=win_send.at[c, o], recv_sem=win_recv.at[c, o],
            device_id=(slab + (o - RANGE), det), device_id_type=MESH,
        )

    def part_copy(c):
        d = order[c]
        return pltpu.make_async_remote_copy(
            src_ref=part.at[c], dst_ref=got_part.at[c],
            send_sem=part_send.at[c], recv_sem=part_recv.at[c],
            device_id=(slab, part_of(d)), device_id_type=MESH,
        )

    def total_copy(c):
        d = order[c]
        return pltpu.make_async_remote_copy(
            src_ref=total, dst_ref=got_total.at[c],
            send_sem=total_send.at[c], recv_sem=total_recv.at[c],
            device_id=(slab, part_of(d)), device_id_type=MESH,
        )

    pl.semaphore_wait(barrier, peers)
    for c in range(n_det):
        for o in away:

            @pl.when(valid(slab + (o - RANGE)))
            def _():
                if c == 0:
                    mask_copy(o).start()
                win_copy(c, o).start()

    for o in away:

        @pl.when(jnp.logical_not(valid(slab - (o - RANGE))))
        def _():
            got_mask[o] = jnp.zeros(got_mask.shape[1:], got_mask.dtype)
            for c in range(n_det):
                got_win[c, o] = jnp.zeros(got_win.shape[2:], got_win.dtype)

    for c in range(n_det):
        for o in away:

            @pl.when(valid(slab - (o - RANGE)))
            def _():
                if c == 0:
                    mask_copy(o).wait_recv()
                win_copy(c, o).wait_recv()

        bins = [jnp.zeros((rows, KWIN), jnp.float32) for _ in range(NTAB)]
        for o in range(OFFSETS):
            if o == RANGE:
                win, mask = send_win[part_of(order[c]), o], send_mask
            else:
                win, mask = got_win[c, o], got_mask
            win = win.astype(jnp.float32)
            for t in range(NTAB):
                weight = jnp.concatenate([mask[o, t : t + 1]] * (KWIN // LANES), axis=1)
                bins[t] = bins[t] + weight * win
        for t in range(NTAB):
            part[c, :, t * KWIN : (t + 1) * KWIN] = bins[t].astype(jnp.bfloat16)
        if order[c] != 0:
            part_copy(c).start()

    summed = part[n_det - 1].astype(jnp.float32)
    for c in range(n_det - 1):
        part_copy(c).wait_recv()
        summed = summed + got_part[c].astype(jnp.float32)
    total[...] = summed.astype(jnp.bfloat16)
    for c in range(n_det - 1):
        total_copy(c).start()

    table_load.wait()
    weights = table_buf[...].reshape(NTAB * KWIN, table_buf.shape[2])

    def finish(quarter_sum, d):
        out[pl.ds(pl.multiple_of(part_of(d) * rows, rows), rows), :] = jnp.dot(
            quarter_sum, weights, preferred_element_type=jnp.float32
        )

    finish(total[...], 0)
    nearest = sorted(range(n_det - 1), key=lambda c: min(order[c], n_det - order[c]))
    for c in nearest:
        total_copy(c).wait_recv()
        finish(got_total[c], n_det - order[c])

    for o in away:

        @pl.when(valid(slab + (o - RANGE)))
        def _():
            mask_copy(o).wait_send()
            for c in range(n_det):
                win_copy(c, o).wait_send()

    for c in range(n_det - 1):
        part_copy(c).wait_send()
        total_copy(c).wait_send()


def body(n_slab, n_det, traces, tables, slab_range, table_slot, sample_start):
    _, frames, samp = traces.shape
    voxels = tables.shape[2]
    rows = frames // n_det
    wide = NTAB * KWIN
    mask_rows = -(-NTAB // 8) * 8
    anywhere = pl.BlockSpec(memory_space=pl.ANY)
    scalars = pl.BlockSpec(memory_space=pltpu.SMEM)
    vmem = pl.BlockSpec(memory_space=pltpu.VMEM)
    dma = pltpu.SemaphoreType.DMA
    wins, masks = pl.pallas_call(
        functools.partial(cut_kernel, n_slab),
        out_shape=[
            jax.ShapeDtypeStruct((n_det, OFFSETS, rows, KWIN), jnp.bfloat16),
            jax.ShapeDtypeStruct((OFFSETS, mask_rows, LANES), jnp.float32),
        ],
        in_specs=[pl.BlockSpec(memory_space=pltpu.HBM), scalars],
        out_specs=[vmem, vmem],
        scratch_shapes=[
            pltpu.VMEM((OFFSETS, frames, KWIN + LANES), jnp.float32),
            dma((OFFSETS,)),
        ],
        compiler_params=pltpu.CompilerParams(vmem_limit_bytes=CUT_LIMIT),
    )(traces, jnp.concatenate([slab_range, table_slot, sample_start], axis=1))
    return pl.pallas_call(
        functools.partial(kernel, n_slab, n_det),
        out_shape=jax.ShapeDtypeStruct((frames, voxels), jnp.float32),
        in_specs=[vmem, vmem, anywhere],
        out_specs=vmem,
        scratch_shapes=[
            pltpu.VMEM(tables.shape, jnp.bfloat16),
            pltpu.VMEM((n_det, OFFSETS, rows, KWIN), jnp.bfloat16),
            pltpu.VMEM((OFFSETS, mask_rows, LANES), jnp.float32),
            pltpu.VMEM((n_det, rows, wide), jnp.bfloat16),
            pltpu.VMEM((n_det, rows, wide), jnp.bfloat16),
            pltpu.VMEM((rows, wide), jnp.bfloat16),
            pltpu.VMEM((n_det, rows, wide), jnp.bfloat16),
            dma,
            dma((n_det, OFFSETS)),
            dma((n_det, OFFSETS)),
            dma((OFFSETS,)),
            dma((OFFSETS,)),
            dma((n_det,)),
            dma((n_det,)),
            dma((n_det,)),
            dma((n_det,)),
        ],
        compiler_params=pltpu.CompilerParams(
            collective_id=0, has_side_effects=True, vmem_limit_bytes=16 * 1024 * 1024
        ),
    )(wins, masks, tables)


def solution(mesh):
    placed = (
        P(("slab", "det"), None, None),
        P("slab", None, "det"),
        P(("slab", "det"), None),
        P(("slab", "det"), None),
        P(("slab", "det"), None),
    )
    return jax.shard_map(
        functools.partial(body, mesh.shape["slab"], mesh.shape["det"]),
        mesh=mesh, in_specs=placed, out_specs=P(None, ("slab", "det")), check_vma=False,
    )
```
